32 devices in a mesh: seq: 16 (over z, x, core), head: 2 (over y).
Axes of the slice: x: 2, y: 2, z: 4, core: 2. Of those that a mesh axis runs over, the one named last changes fastest.
Arguments:
- prompt_queries: bfloat16 [2, 4096, 4096], P('head', 'seq'), may hold values from -6 to 6
- prompt_keys: bfloat16 [2, 4096, 4096], P('head', 'seq'), may hold values from -0.52734375 to 0.52734375
- prompt_values: bfloat16 [2, 4096, 4096], P('head', 'seq'), may hold values from -0.75 to 0.75
- log_gate: float32 [2, 4096, 32], P('head', 'seq'), may hold values from -1 to 0, as said below
- lengths: int32 [2], P('head'), may hold values from 1 to 4096
- out_gain: float32 [32, 128], replicated, may hold values from 0.5 to 1.5
- step_queries: bfloat16 [64, 2, 128], P(('head', 'seq')), may hold values from -6 to 6
- step_keys: bfloat16 [64, 2, 128], P(('head', 'seq')), may hold values from -0.52734375 to 0.52734375
- step_values: bfloat16 [64, 2, 128], P(('head', 'seq')), may hold values from -6 to 6
- step_gates: float32 [64, 2], P(('head', 'seq')), may hold values from -0.7 to -0.05
Outputs:
- prefill_out: bfloat16 [2, 4096, 4096], P('head', 'seq')
- step_out: bfloat16 [64, 2, 128], P(('head', 'seq'))
- cache_state: float32 [64, 128, 128], P(('head', 'seq'))
The draws below stay inside these ranges and needn't reach their ends.
Inputs may be any that keep to these rules, and one draw needn't show every extreme that they name: `log_gate`: every entry is negative.
All inputs are finite; a program needn't handle non-finite values.
Results may differ from the reference program's by a relative error of at most 0.0049.
Values sent between devices are 32-bit elements; how exact they have to be, the bound alone decides.
A program may use at most 128 MiB of HBM per device.

```python
import math
import jax
import jax.numpy as jnp
from jax import lax

HEAD_COUNT_TOTAL = 32
KD = 128
VD = 128
GROUP = 256
STEPS = 2
SEQUENCE_COUNT = 2
PROMPT_LENGTH = 4096
N_SEQ = 16


def draw_log_gate(key, part):
    random_subkeys = jax.random.split(jax.random.fold_in(key, 11), 7)
    slow_share = 0.5
    block_total = PROMPT_LENGTH // GROUP
    slow_heads = jax.random.uniform(random_subkeys[0], (HEAD_COUNT_TOTAL,)) < slow_share
    slow_rate = jax.random.uniform(random_subkeys[1], (HEAD_COUNT_TOTAL,), minval=0.2, maxval=1.0) / PROMPT_LENGTH
    fast_rate = jax.random.uniform(random_subkeys[2], (HEAD_COUNT_TOTAL,), minval=0.02, maxval=0.05)
    block_factor = jnp.exp(jax.random.uniform(random_subkeys[6], (SEQUENCE_COUNT, block_total, 1, HEAD_COUNT_TOTAL), minval=math.log(0.08), maxval=math.log(1.6)))
    block_factor = jnp.broadcast_to(block_factor, (SEQUENCE_COUNT, block_total, GROUP, HEAD_COUNT_TOTAL)).reshape(SEQUENCE_COUNT, PROMPT_LENGTH, HEAD_COUNT_TOTAL)
    head_decay_rates = jnp.where(slow_heads[None, None, :], slow_rate[None, None, :], fast_rate[None, None, :] * block_factor)
    gate_spread_level = jax.random.uniform(random_subkeys[3], (SEQUENCE_COUNT, PROMPT_LENGTH, HEAD_COUNT_TOTAL), minval=0.5, maxval=2.0)
    prompt_groups = jax.random.uniform(random_subkeys[4], (SEQUENCE_COUNT, PROMPT_LENGTH, HEAD_COUNT_TOTAL)) < 3.0 / PROMPT_LENGTH
    group_decay_drop = jax.random.uniform(random_subkeys[5], (SEQUENCE_COUNT, PROMPT_LENGTH, HEAD_COUNT_TOTAL), minval=math.log(0.5), maxval=math.log(0.8))
    return (-head_decay_rates * gate_spread_level + jnp.where(prompt_groups, group_decay_drop, 0.0)).astype(jnp.float32)


def draw_prompt_values(key, part):
    random_subkeys = jax.random.split(jax.random.fold_in(key, 23), 2)
    block_total = PROMPT_LENGTH // GROUP
    full_shape = (SEQUENCE_COUNT, block_total, GROUP, HEAD_COUNT_TOTAL, VD)
    block_level = jnp.exp(jax.random.uniform(random_subkeys[0], (SEQUENCE_COUNT, block_total, 1, HEAD_COUNT_TOTAL, 1), minval=-4.0, maxval=0.2))
    base_values = 0.1 * jnp.clip(jax.random.normal(random_subkeys[1], full_shape), -6.0, 6.0)
    return (base_values * block_level).reshape(SEQUENCE_COUNT, PROMPT_LENGTH, HEAD_COUNT_TOTAL * VD).astype(jnp.bfloat16)


def level_of(rng, extent, cuts, least, top_value):
    factor_of = 1.0
    for position, blocks in cuts:
        draws = jax.random.uniform(jax.random.fold_in(jax.random.fold_in(rng, 6), position), (blocks,), jnp.float32, least / len(cuts), top_value / len(cuts))
        factor_of = factor_of * jnp.repeat(jnp.exp(draws), extent[position] // blocks).reshape((-1,) + (1,) * (len(extent) - 1 - position))
    return factor_of


def noise(key, dims, scale, limit, cuts=(), kind=jnp.bfloat16):
    gain = level_of(key, dims, cuts, -0.22, 0.18) if cuts else 1.0
    values = jax.random.normal(key, dims, jnp.float32) * scale * gain
    return jnp.minimum(jnp.maximum(values, -limit), limit).astype(kind)


def setup_inputs(seed: int = 0) -> dict:
    key_list = jax.random.split(jax.random.key(seed), 11)
    return {
        "prompt_queries": noise(key_list[0], (SEQUENCE_COUNT, PROMPT_LENGTH, HEAD_COUNT_TOTAL * KD), 1.0, 6.0, ((0, 2), (1, 16))),
        "prompt_keys": noise(key_list[1], (SEQUENCE_COUNT, PROMPT_LENGTH, HEAD_COUNT_TOTAL * KD), (KD ** -0.5), 0.52734375, ((0, 2), (1, 16))),
        "prompt_values": draw_prompt_values(jax.random.fold_in(key_list[10], 71), 0),
        "log_gate": draw_log_gate(jax.random.fold_in(key_list[10], 71), 0),
        "lengths": jax.random.randint(key_list[4], (SEQUENCE_COUNT,), 1, PROMPT_LENGTH + 1).astype(jnp.int32),
        "out_gain": jnp.clip(1.0 + 0.1 * jax.random.normal(key_list[5], (HEAD_COUNT_TOTAL, VD), jnp.float32), 0.5, 1.5),
        "step_queries": noise(key_list[6], (HEAD_COUNT_TOTAL * SEQUENCE_COUNT, STEPS, KD), 1.0, 6.0, ((0, 32),)),
        "step_keys": noise(key_list[7], (HEAD_COUNT_TOTAL * SEQUENCE_COUNT, STEPS, KD), (KD ** -0.5), 0.52734375, ((0, 32),)),
        "step_values": noise(key_list[8], (HEAD_COUNT_TOTAL * SEQUENCE_COUNT, STEPS, VD), 1.0, 6.0, ((0, 32),)),
        "step_gates": jnp.clip(-0.7 + 0.65 * jax.random.uniform(key_list[9], (HEAD_COUNT_TOTAL * SEQUENCE_COUNT, STEPS), jnp.float32) ** level_of(key_list[9], (HEAD_COUNT_TOTAL * SEQUENCE_COUNT, STEPS), ((0, 32),), -0.2, 0.2), -0.7, -0.05),
    }


def head_norm(readout, gain_rows):
    power = lax.optimization_barrier(jnp.mean(readout * readout, axis=-1, keepdims=True))
    return readout * lax.rsqrt(power + 1e-06) * gain_rows

def reference(prompt_queries, prompt_keys, prompt_values, log_gate, lengths, out_gain, step_queries, step_keys, step_values, step_gates):
    highest_precision = lax.Precision.HIGHEST
    causal = jnp.arange(GROUP)[:, None] >= jnp.arange(GROUP)[None, :]

    def one_sequence(members):
        queries_all, keys_all, values_all, gates_all, length_one = members
        valid_rows = jnp.arange(PROMPT_LENGTH) < length_one
        gates_all = jnp.where(valid_rows[:, None], gates_all, 0.0)
        keys_all = jnp.where(valid_rows[:, None], keys_all, jnp.zeros_like(keys_all))
        blocks = (queries_all.reshape(N_SEQ, GROUP, HEAD_COUNT_TOTAL, KD), keys_all.reshape(N_SEQ, GROUP, HEAD_COUNT_TOTAL, KD), values_all.reshape(N_SEQ, GROUP, HEAD_COUNT_TOTAL, VD), gates_all.reshape(N_SEQ, GROUP, HEAD_COUNT_TOTAL), valid_rows.reshape(N_SEQ, GROUP))

        def advance(carried_state, block_items):
            queries, keys_kept, values, gates, valid_block = block_items
            cumulative_gates = jnp.cumsum(gates, axis=0)
            totals = cumulative_gates[-1]
            query_wide_float = queries.astype(jnp.float32)
            key_float = keys_kept.astype(jnp.float32)
            value_wide_float = values.astype(jnp.float32)
            cross_group_output = jnp.einsum('lfp,fpx->lfx', query_wide_float * jnp.exp(cumulative_gates)[:, :, None], carried_state, precision=highest_precision)
            scores = jnp.einsum('chk,shk->hcs', query_wide_float, key_float, precision=highest_precision)
            leading = cumulative_gates.T
            spread = leading[:, :, None] - leading[:, None, :]
            decays = jnp.exp(jnp.where(causal[None], spread, -jnp.inf))
            weights = (scores * decays).astype(jnp.bfloat16)
            intra_part = jnp.einsum('hcs,shv->chv', weights.astype(jnp.float32), value_wide_float, precision=highest_precision)
            normed = head_norm(cross_group_output + intra_part, out_gain)
            block_out = jnp.where(valid_block[:, None, None], normed, 0.0).astype(jnp.bfloat16)
            decay_scaled_keys = (key_float * jnp.exp(totals[None, :] - cumulative_gates)[:, :, None]).astype(jnp.bfloat16)
            group_local_state = jnp.einsum('tgb,tgj->gbj', decay_scaled_keys.astype(jnp.float32), value_wide_float, precision=highest_precision)
            carried_state = jnp.exp(totals)[:, None, None] * carried_state + group_local_state
            return (carried_state, block_out)
        final_state, outputs = lax.scan(advance, jnp.zeros((HEAD_COUNT_TOTAL, KD, VD), jnp.float32), blocks)
        return (outputs.reshape(PROMPT_LENGTH, HEAD_COUNT_TOTAL * VD), final_state)
    prefill_out, finals = lax.map(one_sequence, (prompt_queries, prompt_keys, prompt_values, log_gate, lengths))
    cache_now = jnp.transpose(finals, (1, 0, 2, 3)).reshape(HEAD_COUNT_TOTAL * SEQUENCE_COUNT, KD, VD)
    gain_rows = jnp.repeat(out_gain, SEQUENCE_COUNT, axis=0)
    readouts = []
    for decode_step in range(STEPS):
        key_float = step_keys[:, decode_step].astype(jnp.float32)
        value_wide_float = step_values[:, decode_step].astype(jnp.float32)
        cache_now = jnp.exp(step_gates[:, decode_step])[:, None, None] * cache_now + key_float[:, :, None] * value_wide_float[:, None, :]
        reading = jnp.einsum('pk,pkv->pv', step_queries[:, decode_step].astype(jnp.float32), cache_now, precision=highest_precision)
        readouts.append(head_norm(reading, gain_rows).astype(jnp.bfloat16))
    step_out = jnp.stack(readouts, axis=1)
    return (prefill_out, step_out, cache_now)
```

```python
import functools
import jax
import jax.numpy as jnp
from jax import lax
from jax.experimental import pallas as pl
from jax.experimental.pallas import tpu as pltpu
from jax.sharding import PartitionSpec as P

MESH = pl.DeviceIdType.MESH
F32 = jnp.float32
BF16 = jnp.bfloat16
LAG = 3
CHUNK = 4


def column(ref, h):
    wide = ref[...]
    lane = lax.broadcasted_iota(jnp.int32, wide.shape, 1)
    return jnp.sum(jnp.where(lane == h, wide, 0.0), axis=1, keepdims=True)


def head_norm(readout, gain_row):
    power = jnp.mean(readout * readout, axis=-1, keepdims=True)
    return readout * lax.rsqrt(power + 1e-06) * gain_row


def kernel(
    n_seq, n_head,
    len_ref, sgate_ref, q_hbm, k_hbm, v_hbm, gate_ref, gain_ref, sq_ref, sk_ref, sv_ref,
    out_hbm, step_ref, cache_ref,
    q_vm, k_vm, v_vm, o_vm, cum, cum_t, dec, a_own, a_oth, x_own, x_nbr, p_in, p_out,
    i_own, i_oth, i_rcv, fin,
    load_sem, out_sem, dec_s, dec_r, a_s, a_r, x_s, x_r, z_s, z_r, i_s, i_r, f_s, f_r,
):
    group = k_vm.shape[0]
    heads = gate_ref.shape[2]
    half = heads // 2
    kd = k_vm.shape[1] // heads
    vd = v_vm.shape[1] // heads
    rows = fin.shape[0]
    seq = lax.axis_index("seq")
    hd = lax.axis_index("head")
    planes = n_seq // 4
    core = seq % 2
    xx = (seq // 2) % 2
    zz = seq // 4
    place = seq % 4
    base = seq - place
    mate = base + 2 * xx + (1 - core)
    across = base + 2 * (1 - xx) + core
    diagonal = base + 2 * (1 - xx) + (1 - core)
    own0 = core * half
    oth0 = (1 - core) * half

    def owner_of(i):
        row = (own0 + i) * n_head + hd
        dev = row // rows
        return dev // n_seq, dev % n_seq, row % rows

    def source_of(p):
        row = (hd * n_seq + seq) * rows + p
        h = row // n_head
        s = (planes - 1) * 4 + ((h % half) % 2) * 2 + h // half
        return s, row % n_head, h

    def loads(h, which):
        width = CHUNK * kd
        at = pl.ds(pl.multiple_of(h * kd, width), width)
        c = h // CHUNK
        src, dst = ((k_hbm, k_vm), (v_hbm, v_vm), (q_hbm, q_vm))[which]
        return pltpu.make_async_copy(src.at[0, :, at], dst.at[:, at], load_sem.at[which, c])

    for c in range(half // CHUNK):
        for first in (oth0, own0):
            loads(first + c * CHUNK, 0).start()
            loads(first + c * CHUNK, 1).start()
    for c in range(half // CHUNK):
        for first in (oth0, own0):
            loads(first + c * CHUNK, 2).start()

    barrier = pltpu.get_barrier_semaphore()
    for other in (mate, across, diagonal):
        pl.semaphore_signal(barrier, inc=1, device_id={"seq": other, "head": hd}, device_id_type=MESH)

    @pl.when(zz > 0)
    def _():
        pl.semaphore_signal(barrier, inc=1, device_id={"seq": seq - 4, "head": hd}, device_id_type=MESH)

    for p in range(rows):
        s, b, _h = source_of(p)

        @pl.when(jnp.logical_or(s != seq, b != hd))
        def _():
            pl.semaphore_signal(barrier, inc=1, device_id={"seq": s, "head": b}, device_id_type=MESH)

    start = seq * group
    length = len_ref[0]
    valid_col = (lax.broadcasted_iota(jnp.int32, (group, 1), 0) + start) < length
    t_iota = lax.broadcasted_iota(jnp.int32, (group, group), 0)
    s_iota = lax.broadcasted_iota(jnp.int32, (group, group), 1)
    gates = jnp.where(valid_col, gate_ref[0], 0.0)
    tril = (t_iota >= s_iota).astype(F32)
    cumulative = jnp.dot(tril, gates, precision=lax.Precision.HIGHEST, preferred_element_type=F32)
    cum[...] = cumulative
    turned = cumulative.T
    cum_t[...] = turned
    dec[place] = jnp.exp(jnp.broadcast_to(turned[:, group - 1:group], (heads, vd)))

    @pl.when(zz == 0)
    def _():
        p_in[...] = jnp.zeros_like(p_in)

    last = zz == planes - 1
    greeted = 0
    for i in range(half):
        oh, os_, _slot = owner_of(i)
        sends = jnp.logical_and(xx == i % 2, jnp.logical_or(oh != hd, os_ != seq))
        greeted = greeted + jnp.where(sends, 1, 0)
    pl.semaphore_wait(barrier, 3 + jnp.where(last, greeted, 1))

    def dec_copy(n, other):
        return pltpu.make_async_remote_copy(
            src_ref=dec.at[place], dst_ref=dec.at[place], send_sem=dec_s.at[n],
            recv_sem=dec_r.at[place], device_id={"seq": other, "head": hd}, device_id_type=MESH)

    def dec_arrival(other):
        slot = other % 4
        return pltpu.make_async_remote_copy(
            src_ref=dec.at[slot], dst_ref=dec.at[slot], send_sem=dec_s.at[0],
            recv_sem=dec_r.at[slot], device_id={"seq": other, "head": hd}, device_id_type=MESH)

    for n, other in enumerate((mate, across, diagonal)):
        dec_copy(n, other).start()

    def send(src, dst, ssem, rsem, s, h=None):
        return pltpu.make_async_remote_copy(
            src_ref=src, dst_ref=dst, send_sem=ssem, recv_sem=rsem,
            device_id={"seq": s, "head": hd if h is None else h}, device_id_type=MESH)

    def a_copy(i):
        return send(a_own.at[oth0 + i], a_oth.at[i], a_s.at[i], a_r.at[i], mate)

    def x_copy(i):
        return send(x_own.at[i], x_nbr.at[i], x_s.at[i], x_r.at[i], across)

    def z_copy(i):
        return send(p_out.at[i], p_in.at[i], z_s.at[i], z_r.at[i], jnp.minimum(seq + 4, n_seq - 4 + place))

    def i_copy(i):
        return send(i_oth.at[i], i_rcv.at[i], i_s.at[i], i_r.at[i], mate)

    def f_copy(i):
        oh, os_, slot = owner_of(i)
        return send(p_out.at[i], fin.at[slot], f_s.at[i], f_r.at[slot], os_, oh)

    def lanes(h):
        return pl.ds(pl.multiple_of(h * kd, kd), kd)

    def local_state(h):
        col = column(cum, h)
        scale = jnp.where(valid_col, jnp.exp(col[group - 1:group, :] - col), 0.0)
        wk = (k_vm[:, lanes(h)].astype(F32) * scale).astype(BF16)
        a_own[h] = lax.dot_general(
            wk, v_vm[:, lanes(h)], (((0,), (0,)), ((), ())), preferred_element_type=F32)

    def wait_loads(i, which):
        @pl.when(i % CHUNK == 0)
        def _():
            c = i // CHUNK * CHUNK
            for w in which:
                loads(oth0 + c, w).wait()
                loads(own0 + c, w).wait()

    def produce(i):
        wait_loads(i, (0, 1))
        local_state(oth0 + i)
        a_copy(i).start()
        local_state(own0 + i)

    def chip_parts(i):
        h = own0 + i
        mine, theirs = a_own[h], a_oth[i]
        early = jnp.where(core == 0, mine, theirs)
        late = jnp.where(core == 0, theirs, mine)
        return early, late

    def combine(i):
        h = own0 + i
        a_copy(i).wait_recv()
        early, late = chip_parts(i)
        x_own[i] = early * dec[2 * xx + 1, pl.ds(h, 1), :] + late
        x_copy(i).start()

    def loop(lo, hi, body):
        def step(i, c):
            body(i)
            return c
        lax.fori_loop(lo, hi, step, 0)

    loop(0, LAG, produce)
    for other in (mate, across, diagonal):
        dec_arrival(other).wait_recv()

    def both(i):
        produce(i)
        combine(i - LAG)

    loop(LAG, half, both)
    loop(half - LAG, half, combine)

    def chain(i):
        h = own0 + i
        x_copy(i).wait_recv()

        @pl.when(zz > 0)
        def _():
            z_copy(i).wait_recv()

        first = xx == 0
        mine, theirs = x_own[i], x_nbr[i]
        d0 = dec[0, pl.ds(h, 1), :] * dec[1, pl.ds(h, 1), :]
        d1 = dec[2, pl.ds(h, 1), :] * dec[3, pl.ds(h, 1), :]
        entering = p_in[i]
        middle = entering * d0 + jnp.where(first, mine, theirs)
        p_out[i] = middle * d1 + jnp.where(first, theirs, mine)

        @pl.when(zz < planes - 1)
        def _():
            z_copy(i).start()

        @pl.when(jnp.logical_and(zz == planes - 1, xx == i % 2))
        def _():
            oh, os_, slot = owner_of(i)
            away = jnp.logical_or(oh != hd, os_ != seq)

            @pl.when(away)
            def _():
                f_copy(i).start()

            @pl.when(jnp.logical_not(away))
            def _():
                fin[slot] = p_out[i]

        early, _late = chip_parts(i)
        into0 = jnp.where(first, entering, middle)
        into1 = into0 * dec[2 * xx, pl.ds(h, 1), :] + early
        i_oth[i] = jnp.where(core == 0, into1, into0)
        i_copy(i).start()
        i_own[i] = jnp.where(core == 0, into0, into1)

    valid_row = (lax.broadcasted_iota(jnp.int32, (1, group), 1) + start) < length

    def out_copy(h):
        return pltpu.make_async_copy(o_vm.at[:, lanes(h)], out_hbm.at[0, :, lanes(h)], out_sem.at[h])

    def head_out(h, state):
        q = q_vm[:, lanes(h)]
        scores = lax.dot_general(
            q, k_vm[:, lanes(h)], (((1,), (1,)), ((), ())), preferred_element_type=F32)
        col = column(cum, h)
        spread = col - cum_t[pl.ds(h, 1), :]
        t_pos = lax.broadcasted_iota(jnp.int32, (group, group), 0)
        s_pos = lax.broadcasted_iota(jnp.int32, (group, group), 1)
        keep = jnp.logical_and(t_pos >= s_pos, valid_row)
        weights = (scores * jnp.exp(jnp.where(keep, spread, -jnp.inf))).astype(BF16)
        intra = jnp.dot(weights, v_vm[:, lanes(h)], preferred_element_type=F32)
        inter = jnp.exp(col) * jnp.dot(q, state.astype(BF16), preferred_element_type=F32)
        normed = head_norm(inter + intra, gain_ref[pl.ds(h, 1), :])
        o_vm[:, lanes(h)] = jnp.where(valid_col, normed, 0.0).astype(BF16)
        out_copy(h).start()

    def other_out(i):
        i_copy(i).wait_recv()
        head_out(oth0 + i, i_rcv[i])

    def first_round(i):
        wait_loads(i, (2,))
        chain(i)
        head_out(own0 + i, i_own[i])

    def later_round(i):
        first_round(i)
        other_out(i - 1)

    loop(0, 1, first_round)
    loop(1, half, later_round)
    other_out(half - 1)

    for p in range(rows):
        s, b, h = source_of(p)

        @pl.when(jnp.logical_or(s != seq, b != hd))
        def _():
            send(fin.at[p], fin.at[p], f_s.at[0], f_r.at[p], s, b).wait_recv()

        gain_row = gain_ref[pl.ds(h, 1), :]
        sk, sv, sq = sk_ref[p].astype(F32), sv_ref[p].astype(F32), sq_ref[p].astype(F32)
        now = fin[p]
        outs = []
        for j in range(sk.shape[0]):
            kcol = jnp.broadcast_to(sk[j:j + 1, :], (vd, kd)).T
            qcol = jnp.broadcast_to(sq[j:j + 1, :], (vd, kd)).T
            now = jnp.exp(jnp.full((1, vd), sgate_ref[p, j], F32)) * now + kcol * sv[j:j + 1, :]
            outs.append(head_norm(jnp.sum(qcol * now, axis=0, keepdims=True), gain_row))
        step_ref[p] = jnp.concatenate(outs, axis=0).astype(BF16)
        cache_ref[p] = now

    for n, other in enumerate((mate, across, diagonal)):
        dec_copy(n, other).wait_send()

    def drain(i):
        a_copy(i).wait_send()
        x_copy(i).wait_send()
        i_copy(i).wait_send()
        out_copy(own0 + i).wait()
        out_copy(oth0 + i).wait()

        @pl.when(zz < planes - 1)
        def _():
            z_copy(i).wait_send()

        @pl.when(jnp.logical_and(zz == planes - 1, xx == i % 2))
        def _():
            oh, os_, _slot = owner_of(i)

            @pl.when(jnp.logical_or(oh != hd, os_ != seq))
            def _():
                f_copy(i).wait_send()

    loop(0, half, drain)


def per_device(n_seq, n_head, pq, pk, pv, lg, ln, gain, sq, sk, sv, sg):
    batch, group, width = pq.shape
    assert batch == 1 and n_seq % 4 == 0
    heads = lg.shape[2]
    half = heads // 2
    kd = width // heads
    vd = gain.shape[1]
    rows = sq.shape[0]
    vm = pl.BlockSpec(memory_space=pltpu.VMEM)
    sm = pl.BlockSpec(memory_space=pltpu.SMEM)
    anyw = pl.BlockSpec(memory_space=pl.ANY)
    state = lambda n: pltpu.VMEM((n, kd, vd), F32)
    dma = lambda *n: pltpu.SemaphoreType.DMA(n)
    return pl.pallas_call(
        functools.partial(kernel, n_seq, n_head),
        out_shape=(
            jax.ShapeDtypeStruct((batch, group, heads * vd), BF16),
            jax.ShapeDtypeStruct(sv.shape, BF16),
            jax.ShapeDtypeStruct((rows, kd, vd), F32),
        ),
        in_specs=[sm, sm, anyw, anyw, anyw, vm, vm, vm, vm, vm],
        out_specs=(anyw, vm, vm),
        scratch_shapes=[
            pltpu.VMEM((group, width), BF16),
            pltpu.VMEM((group, width), BF16),
            pltpu.VMEM((group, heads * vd), BF16),
            pltpu.VMEM((group, heads * vd), BF16),
            pltpu.VMEM((group, heads), F32),
            pltpu.VMEM((heads, group), F32),
            pltpu.VMEM((4, heads, vd), F32),
            state(heads), state(half), state(half), state(half), state(half), state(half),
            state(half), state(half), state(half), state(rows),
            dma(3, heads // CHUNK), dma(heads), dma(3), dma(4),
            dma(half), dma(half), dma(half), dma(half), dma(half), dma(half),
            dma(half), dma(half), dma(half), dma(rows),
        ],
        compiler_params=pltpu.CompilerParams(
            collective_id=0, has_side_effects=True, vmem_limit_bytes=48 * 1024 * 1024),
    )(ln, sg, pq, pk, pv, lg, gain, sq, sk, sv)


def solution(mesh):
    return jax.shard_map(
        functools.partial(per_device, mesh.shape["seq"], mesh.shape["head"]),
        mesh=mesh,
        in_specs=(
            P("head", "seq", None),
            P("head", "seq", None),
            P("head", "seq", None),
            P("head", "seq", None),
            P("head"),
            P(),
            P(("head", "seq"), None, None),
            P(("head", "seq"), None, None),
            P(("head", "seq"), None, None),
            P(("head", "seq"), None),
        ),
        out_specs=(
            P("head", "seq", None),
            P(("head", "seq"), None, None),
            P(("head", "seq"), None, None),
        ),
        check_vma=False,
    )
```

```python
import functools
import jax
import jax.numpy as jnp
from jax import lax
from jax.experimental import pallas as pl
from jax.experimental.pallas import tpu as pltpu
from jax.sharding import PartitionSpec as P

MESH = pl.DeviceIdType.MESH
F32 = jnp.float32
BF16 = jnp.bfloat16
LAG = 2
CHUNK = 4


def column(ref, h):
    wide = ref[...]
    lane = lax.broadcasted_iota(jnp.int32, wide.shape, 1)
    return jnp.sum(jnp.where(lane == h, wide, 0.0), axis=1, keepdims=True)


def head_norm(readout, gain_row):
    power = jnp.mean(readout * readout, axis=-1, keepdims=True)
    return readout * lax.rsqrt(power + 1e-06) * gain_row


def kernel(
    n_seq, n_head,
    len_ref, q_hbm, k_hbm, v_hbm, gate_hbm, gain_hbm, sq_hbm, sk_hbm, sv_hbm, sg_hbm,
    o_vm, step_ref, cache_ref,
    q_vm, k_vm, v_vm, gate_ref, gain_ref, sq_ref, sk_ref, sv_ref, sgate_ref, intra, cum, cum_t, dec, a_own, a_oth, x_own, x_nbr, p_in, p_out,
    i_own, i_oth, i_rcv, fin,
    load_sem, small_sem, dec_s, dec_r, a_s, a_r, x_s, x_r, z_s, z_r, i_s, i_r, f_s, f_r,
):
    group = k_vm.shape[0]
    heads = gate_ref.shape[1]
    half = heads // 2
    kd = k_vm.shape[1] // heads
    vd = v_vm.shape[1] // heads
    rows = fin.shape[0]
    seq = lax.axis_index("seq")
    hd = lax.axis_index("head")
    planes = n_seq // 4
    core = seq % 2
    xx = (seq // 2) % 2
    zz = seq // 4
    place = seq % 4
    base = seq - place
    mate = base + 2 * xx + (1 - core)
    across = base + 2 * (1 - xx) + core
    diagonal = base + 2 * (1 - xx) + (1 - core)
    own0 = core * half
    oth0 = (1 - core) * half

    def owner_of(i):
        row = (own0 + i) * n_head + hd
        dev = row // rows
        return dev // n_seq, dev % n_seq, row % rows

    def source_of(p):
        row = (hd * n_seq + seq) * rows + p
        h = row // n_head
        s = (planes - 1) * 4 + ((h % half) % 2) * 2 + h // half
        return s, row % n_head, h

    def loads(h, which):
        width = CHUNK * kd
        at = pl.ds(pl.multiple_of(h * kd, width), width)
        c = h // CHUNK
        src, dst = ((k_hbm, k_vm), (v_hbm, v_vm), (q_hbm, q_vm))[which]
        return pltpu.make_async_copy(src.at[0, :, at], dst.at[:, at], load_sem.at[which, c])

    small = [
        pltpu.make_async_copy(src, dst, small_sem.at[n])
        for n, (src, dst) in enumerate((
            (gate_hbm, gate_ref), (gain_hbm, gain_ref), (sq_hbm, sq_ref), (sk_hbm, sk_ref),
            (sv_hbm, sv_ref), (sg_hbm, sgate_ref)))
    ]
    for copy in small:
        copy.start()
    for c in range(half // CHUNK):
        for first in (oth0, own0):
            loads(first + c * CHUNK, 0).start()
            loads(first + c * CHUNK, 1).start()
    for c in range(half // CHUNK):
        for first in (oth0, own0):
            loads(first + c * CHUNK, 2).start()

    barrier = pltpu.get_barrier_semaphore()
    for other in (mate, across, diagonal):
        pl.semaphore_signal(barrier, inc=1, device_id={"seq": other, "head": hd}, device_id_type=MESH)

    @pl.when(zz > 0)
    def _():
        pl.semaphore_signal(barrier, inc=1, device_id={"seq": seq - 4, "head": hd}, device_id_type=MESH)

    for p in range(rows):
        s, b, _h = source_of(p)

        @pl.when(jnp.logical_or(s != seq, b != hd))
        def _():
            pl.semaphore_signal(barrier, inc=1, device_id={"seq": s, "head": b}, device_id_type=MESH)

    start = seq * group
    length = len_ref[0]
    valid_col = (lax.broadcasted_iota(jnp.int32, (group, 1), 0) + start) < length
    t_iota = lax.broadcasted_iota(jnp.int32, (group, group), 0)
    s_iota = lax.broadcasted_iota(jnp.int32, (group, group), 1)
    valid_row = (lax.broadcasted_iota(jnp.int32, (1, group), 1) + start) < length
    small[0].wait()
    gates = jnp.where(valid_row, gate_ref[0], 0.0)
    triu = (t_iota <= s_iota).astype(F32)
    turned = jnp.dot(gates, triu, precision=lax.Precision.HIGHEST, preferred_element_type=F32)
    cum_t[...] = turned
    cum[...] = turned.T
    dec[place] = jnp.exp(jnp.broadcast_to(turned[:, group - 1:group], (heads, vd)))

    @pl.when(zz == 0)
    def _():
        p_in[...] = jnp.zeros_like(p_in)

    last = zz == planes - 1
    greeted = 0
    for i in range(half):
        oh, os_, _slot = owner_of(i)
        sends = jnp.logical_and(xx == i % 2, jnp.logical_or(oh != hd, os_ != seq))
        greeted = greeted + jnp.where(sends, 1, 0)
    pl.semaphore_wait(barrier, 3 + jnp.where(last, greeted, 1))

    def dec_copy(n, other):
        return pltpu.make_async_remote_copy(
            src_ref=dec.at[place], dst_ref=dec.at[place], send_sem=dec_s.at[n],
            recv_sem=dec_r.at[place], device_id={"seq": other, "head": hd}, device_id_type=MESH)

    def dec_arrival(other):
        slot = other % 4
        return pltpu.make_async_remote_copy(
            src_ref=dec.at[slot], dst_ref=dec.at[slot], send_sem=dec_s.at[0],
            recv_sem=dec_r.at[slot], device_id={"seq": other, "head": hd}, device_id_type=MESH)

    for n, other in enumerate((mate, across, diagonal)):
        dec_copy(n, other).start()

    def send(src, dst, ssem, rsem, s, h=None):
        return pltpu.make_async_remote_copy(
            src_ref=src, dst_ref=dst, send_sem=ssem, recv_sem=rsem,
            device_id={"seq": s, "head": hd if h is None else h}, device_id_type=MESH)

    def a_copy(i):
        return send(a_own.at[oth0 + i], a_oth.at[i], a_s.at[i], a_r.at[i], mate)

    def part(r):
        return pl.ds(r * (kd // 2), kd // 2)

    def x_copy(i, r):
        n = 2 * i + r
        return send(x_own.at[i, part(r)], x_nbr.at[i, part(r)], x_s.at[n], x_r.at[n], across)

    def z_copy(i, r):
        n = 2 * i + r
        return send(p_out.at[i, part(r)], p_in.at[i, part(r)], z_s.at[n], z_r.at[n],
                    jnp.minimum(seq + 4, n_seq - 4 + place))

    def i_copy(i):
        return send(i_oth.at[i], i_rcv.at[i], i_s.at[i], i_r.at[i], mate)

    def f_copy(i):
        oh, os_, slot = owner_of(i)
        return send(p_out.at[i], fin.at[slot], f_s.at[i], f_r.at[slot], os_, oh)

    def lanes(h):
        return pl.ds(pl.multiple_of(h * kd, kd), kd)

    def local_state(h):
        col = column(cum, h)
        scale = jnp.where(valid_col, jnp.exp(col[group - 1:group, :] - col), 0.0)
        wk = (k_vm[:, lanes(h)].astype(F32) * scale).astype(BF16)
        return lax.dot_general(
            wk, v_vm[:, lanes(h)], (((0,), (0,)), ((), ())), preferred_element_type=F32)

    def wait_loads(i, which):
        @pl.when(i % CHUNK == 0)
        def _():
            c = i // CHUNK * CHUNK
            for w in which:
                loads(oth0 + c, w).wait()
                loads(own0 + c, w).wait()

    def produce(i):
        wait_loads(i, (0, 1))
        one, two = local_state(oth0 + i), local_state(own0 + i)
        a_own[oth0 + i] = one
        a_copy(i).start()
        a_own[own0 + i] = two

    def combine(i):
        h = own0 + i
        a_copy(i).wait_recv()
        mine, theirs = a_own[h], a_oth[i]
        early = jnp.where(core == 0, mine, theirs)
        late = jnp.where(core == 0, theirs, mine)
        x_own[i] = early * dec[2 * xx + 1, pl.ds(h, 1), :] + late
        for r in range(2):
            x_copy(i, r).start()

    def chain(i, r):
        h = own0 + i
        x_copy(i, r).wait_recv()

        @pl.when(zz > 0)
        def _():
            z_copy(i, r).wait_recv()

        first = xx == 0
        at = part(r)
        mine, theirs = x_own[i, at], x_nbr[i, at]
        d0 = dec[0, pl.ds(h, 1), :] * dec[1, pl.ds(h, 1), :]
        d1 = dec[2, pl.ds(h, 1), :] * dec[3, pl.ds(h, 1), :]
        entering = p_in[i, at]
        middle = entering * d0 + jnp.where(first, mine, theirs)
        p_out[i, at] = middle * d1 + jnp.where(first, theirs, mine)

        @pl.when(zz < planes - 1)
        def _():
            z_copy(i, r).start()

        if r == 1:
            @pl.when(jnp.logical_and(zz == planes - 1, xx == i % 2))
            def _():
                oh, os_, slot = owner_of(i)
                away = jnp.logical_or(oh != hd, os_ != seq)

                @pl.when(away)
                def _():
                    f_copy(i).start()

                @pl.when(jnp.logical_not(away))
                def _():
                    fin[slot] = p_out[i]

        early = jnp.where(core == 0, a_own[h, at], a_oth[i, at])
        into0 = jnp.where(first, entering, middle)
        into1 = into0 * dec[2 * xx, pl.ds(h, 1), :] + early
        i_oth[i, at] = jnp.where(core == 0, into1, into0)
        if r == 1:
            i_copy(i).start()
        i_own[i, at] = jnp.where(core == 0, into0, into1)

    def inside(h):
        scores = lax.dot_general(
            q_vm[:, lanes(h)], k_vm[:, lanes(h)], (((1,), (1,)), ((), ())),
            preferred_element_type=F32)
        spread = column(cum, h) - cum_t[pl.ds(h, 1), :]
        t_pos = lax.broadcasted_iota(jnp.int32, (group, group), 0)
        s_pos = lax.broadcasted_iota(jnp.int32, (group, group), 1)
        keep = jnp.logical_and(t_pos >= s_pos, valid_row)
        weights = (scores * jnp.exp(jnp.where(keep, spread, -jnp.inf))).astype(BF16)
        return jnp.dot(weights, v_vm[:, lanes(h)], preferred_element_type=F32)

    def inside_pair(i):
        wait_loads(i, (2,))
        one, two = inside(own0 + i), inside(oth0 + i)
        intra[own0 + i] = one
        intra[oth0 + i] = two

    def finish(h, state):
        inter = jnp.exp(column(cum, h)) * jnp.dot(
            q_vm[:, lanes(h)], state.astype(BF16), preferred_element_type=F32)
        normed = head_norm(inter + intra[h], gain_ref[pl.ds(h, 1), :])
        return jnp.where(valid_col, normed, 0.0).astype(BF16)

    def put(h, block):
        o_vm[0, :, lanes(h)] = block

    lag = 4 + 2 * jnp.minimum(zz, 3)

    def round_of(n, c):
        i = n - lag
        running = jnp.logical_and(i >= 0, i < half)

        @pl.when(n < half)
        def _():
            produce(n)

        @pl.when(n == LAG - 1)
        def _():
            for other in (mate, across, diagonal):
                dec_arrival(other).wait_recv()

        @pl.when(jnp.logical_and(n >= LAG, n < half + LAG))
        def _():
            combine(n - LAG)

        @pl.when(running)
        def _():
            chain(i, 0)

        @pl.when(n < half)
        def _():
            inside_pair(n)

        @pl.when(running)
        def _():
            chain(i, 1)

        @pl.when(i == 0)
        def _():
            put(own0, finish(own0, i_own[0]))

        @pl.when(jnp.logical_and(i > 0, i < half))
        def _():
            i_copy(i - 1).wait_recv()
            one = finish(own0 + i, i_own[i])
            two = finish(oth0 + i - 1, i_rcv[i - 1])
            put(own0 + i, one)
            put(oth0 + i - 1, two)

        return c

    for copy in small[1:]:
        copy.wait()
    lax.fori_loop(0, half + lag, round_of, 0)
    i_copy(half - 1).wait_recv()
    put(oth0 + half - 1, finish(oth0 + half - 1, i_rcv[half - 1]))

    for p in range(rows):
        s, b, h = source_of(p)

        @pl.when(jnp.logical_or(s != seq, b != hd))
        def _():
            send(fin.at[p], fin.at[p], f_s.at[0], f_r.at[p], s, b).wait_recv()

        gain_row = gain_ref[pl.ds(h, 1), :]
        sk, sv, sq = sk_ref[p].astype(F32), sv_ref[p].astype(F32), sq_ref[p].astype(F32)
        now = fin[p]
        outs = []
        for j in range(sk.shape[0]):
            kcol = jnp.broadcast_to(sk[j:j + 1, :], (vd, kd)).T
            qcol = jnp.broadcast_to(sq[j:j + 1, :], (vd, kd)).T
            now = jnp.exp(jnp.broadcast_to(sgate_ref[p:p + 1, j:j + 1], (1, vd))) * now + kcol * sv[j:j + 1, :]
            outs.append(head_norm(jnp.sum(qcol * now, axis=0, keepdims=True), gain_row))
        step_ref[p] = jnp.concatenate(outs, axis=0).astype(BF16)
        cache_ref[p] = now

    for n, other in enumerate((mate, across, diagonal)):
        dec_copy(n, other).wait_send()

    def drain(i, c):
        a_copy(i).wait_send()
        i_copy(i).wait_send()
        for r in range(2):
            x_copy(i, r).wait_send()

        @pl.when(zz < planes - 1)
        def _():
            for r in range(2):
                z_copy(i, r).wait_send()

        @pl.when(jnp.logical_and(zz == planes - 1, xx == i % 2))
        def _():
            oh, os_, _slot = owner_of(i)

            @pl.when(jnp.logical_or(oh != hd, os_ != seq))
            def _():
                f_copy(i).wait_send()

        return c

    lax.fori_loop(0, half, drain, 0)


def store_kernel(*refs):
    n = len(refs) // 2
    copies = [pltpu.make_async_copy(refs[j], refs[n + j], refs[-1].at[j]) for j in range(n)]
    for copy in copies:
        copy.start()
    for copy in copies:
        copy.wait()


def per_device(n_seq, n_head, pq, pk, pv, lg, ln, gain, sq, sk, sv, sg):
    batch, group, width = pq.shape
    assert batch == 1 and n_seq % 4 == 0
    heads = lg.shape[2]
    half = heads // 2
    kd = width // heads
    vd = gain.shape[1]
    rows = sq.shape[0]
    vm = pl.BlockSpec(memory_space=pltpu.VMEM)
    sm = pl.BlockSpec(memory_space=pltpu.SMEM)
    far = pl.BlockSpec(memory_space=pltpu.HBM)
    state = lambda n: pltpu.VMEM((n, kd, vd), F32)
    dma = lambda *n: pltpu.SemaphoreType.DMA(n)
    results = pl.pallas_call(
        functools.partial(kernel, n_seq, n_head),
        out_shape=(
            pltpu.VMEM((batch, group, heads * vd), BF16),
            pltpu.VMEM(sv.shape, BF16),
            pltpu.VMEM((rows, kd, vd), F32),
        ),
        in_specs=[sm] + [far] * 9,
        out_specs=(vm, vm, vm),
        scratch_shapes=[
            pltpu.VMEM((group, width), BF16),
            pltpu.VMEM((group, width), BF16),
            pltpu.VMEM((group, heads * vd), BF16),
            pltpu.VMEM((batch, heads, group), F32),
            pltpu.VMEM(gain.shape, F32),
            pltpu.VMEM(sq.shape, BF16),
            pltpu.VMEM(sk.shape, BF16),
            pltpu.VMEM(sv.shape, BF16),
            pltpu.VMEM(sg.shape, F32),
            pltpu.VMEM((heads, group, vd), F32),
            pltpu.VMEM((group, heads), F32),
            pltpu.VMEM((heads, group), F32),
            pltpu.VMEM((4, heads, vd), F32),
            state(heads), state(half), state(half), state(half), state(half), state(half),
            state(half), state(half), state(half), state(rows),
            dma(3, heads // CHUNK), dma(6), dma(3), dma(4),
            dma(half), dma(half), dma(heads), dma(heads), dma(heads), dma(heads),
            dma(half), dma(half), dma(half), dma(rows),
        ],
        compiler_params=pltpu.CompilerParams(
            collective_id=0, has_side_effects=True, vmem_limit_bytes=60 * 1024 * 1024),
    )(ln, pq, pk, pv, jnp.transpose(lg, (0, 2, 1)), gain, sq, sk, sv, sg)
    return pl.pallas_call(
        store_kernel,
        out_shape=tuple(jax.ShapeDtypeStruct(r.shape, r.dtype) for r in results),
        in_specs=[vm] * 3,
        out_specs=(far,) * 3,
        scratch_shapes=[dma(3)],
        compiler_params=pltpu.CompilerParams(vmem_limit_bytes=8 * 1024 * 1024),
    )(*results)


def solution(mesh):
    return jax.shard_map(
        functools.partial(per_device, mesh.shape["seq"], mesh.shape["head"]),
        mesh=mesh,
        in_specs=(
            P("head", "seq", None),
            P("head", "seq", None),
            P("head", "seq", None),
            P("head", "seq", None),
            P("head"),
            P(),
            P(("head", "seq"), None, None),
            P(("head", "seq"), None, None),
            P(("head", "seq"), None, None),
            P(("head", "seq"), None),
        ),
        out_specs=(
            P("head", "seq", None),
            P(("head", "seq"), None, None),
            P(("head", "seq"), None, None),
        ),
        check_vma=False,
    )
```

```python
import functools
import jax
import jax.numpy as jnp
from jax import lax
from jax.experimental import pallas as pl
from jax.experimental.pallas import tpu as pltpu
from jax.sharding import PartitionSpec as P

MESH = pl.DeviceIdType.MESH
F32 = jnp.float32
BF16 = jnp.bfloat16
LAG = 2
AHEAD = 3
CHUNK = 4


def column(ref, h):
    wide = ref[...]
    lane = lax.broadcasted_iota(jnp.int32, wide.shape, 1)
    return jnp.sum(jnp.where(lane == h, wide, 0.0), axis=1, keepdims=True)


def head_norm(readout, gain_row):
    power = jnp.mean(readout * readout, axis=-1, keepdims=True)
    return readout * lax.rsqrt(power + 1e-06) * gain_row


def kernel(
    n_seq, n_head,
    len_ref, q_hbm, k_hbm, v_hbm, gate_hbm, gain_hbm, sq_hbm, sk_hbm, sv_hbm, sg_hbm,
    o_vm, step_ref, cache_ref,
    q_vm, k_vm, v_vm, gate_ref, gain_ref, sq_ref, sk_ref, sv_ref, sgate_ref, intra, cum, cum_t, dec, a_own, a_oth, x_own, x_nbr, p_in, p_out,
    i_own, i_oth, i_rcv, fin,
    load_sem, small_sem, dec_s, dec_r, a_s, a_r, x_s, x_r, z_s, z_r, i_s, i_r, f_s, f_r,
):
    group = k_vm.shape[0]
    heads = gate_ref.shape[1]
    half = heads // 2
    kd = k_vm.shape[1] // heads
    vd = v_vm.shape[1] // heads
    rows = fin.shape[0]
    seq = lax.axis_index("seq")
    hd = lax.axis_index("head")
    planes = n_seq // 4
    core = seq % 2
    xx = (seq // 2) % 2
    zz = seq // 4
    place = seq % 4
    base = seq - place
    mate = base + 2 * xx + (1 - core)
    across = base + 2 * (1 - xx) + core
    diagonal = base + 2 * (1 - xx) + (1 - core)
    own0 = core * half
    oth0 = (1 - core) * half

    def owner_of(i):
        row = (own0 + i) * n_head + hd
        dev = row // rows
        return dev // n_seq, dev % n_seq, row % rows

    def source_of(p):
        row = (hd * n_seq + seq) * rows + p
        h = row // n_head
        s = (planes - 1) * 4 + ((h % half) % 2) * 2 + h // half
        return s, row % n_head, h

    def loads(h, which):
        width = CHUNK * kd
        at = pl.ds(pl.multiple_of(h * kd, width), width)
        c = h // CHUNK
        src, dst = ((k_hbm, k_vm), (v_hbm, v_vm), (q_hbm, q_vm))[which]
        return pltpu.make_async_copy(src.at[0, :, at], dst.at[:, at], load_sem.at[which, c])

    small = [
        pltpu.make_async_copy(src, dst, small_sem.at[n])
        for n, (src, dst) in enumerate((
            (gate_hbm, gate_ref), (gain_hbm, gain_ref), (sq_hbm, sq_ref), (sk_hbm, sk_ref),
            (sv_hbm, sv_ref), (sg_hbm, sgate_ref)))
    ]
    for copy in small:
        copy.start()
    for c in range(half // CHUNK):
        for first in (oth0, own0):
            loads(first + c * CHUNK, 0).start()
            loads(first + c * CHUNK, 1).start()
    for c in range(half // CHUNK):
        for first in (oth0, own0):
            loads(first + c * CHUNK, 2).start()

    barrier = pltpu.get_barrier_semaphore()
    for other in (mate, across, diagonal):
        pl.semaphore_signal(barrier, inc=1, device_id={"seq": other, "head": hd}, device_id_type=MESH)

    @pl.when(zz > 0)
    def _():
        pl.semaphore_signal(barrier, inc=1, device_id={"seq": seq - 4, "head": hd}, device_id_type=MESH)

    for p in range(rows):
        s, b, _h = source_of(p)

        @pl.when(jnp.logical_or(s != seq, b != hd))
        def _():
            pl.semaphore_signal(barrier, inc=1, device_id={"seq": s, "head": b}, device_id_type=MESH)

    start = seq * group
    length = len_ref[0]
    valid_col = (lax.broadcasted_iota(jnp.int32, (group, 1), 0) + start) < length
    t_iota = lax.broadcasted_iota(jnp.int32, (group, group), 0)
    s_iota = lax.broadcasted_iota(jnp.int32, (group, group), 1)
    valid_row = (lax.broadcasted_iota(jnp.int32, (1, group), 1) + start) < length
    small[0].wait()
    gates = jnp.where(valid_row, gate_ref[0], 0.0)
    triu = (t_iota <= s_iota).astype(F32)
    turned = jnp.dot(gates, triu, precision=lax.Precision.HIGHEST, preferred_element_type=F32)
    cum_t[...] = turned
    cum[...] = turned.T
    dec[place] = jnp.exp(jnp.broadcast_to(turned[:, group - 1:group], (heads, vd)))

    @pl.when(zz == 0)
    def _():
        p_in[...] = jnp.zeros_like(p_in)

    last = zz == planes - 1
    greeted = 0
    for i in range(half):
        oh, os_, _slot = owner_of(i)
        sends = jnp.logical_and(xx == i % 2, jnp.logical_or(oh != hd, os_ != seq))
        greeted = greeted + jnp.where(sends, 1, 0)
    pl.semaphore_wait(barrier, 3 + jnp.where(last, greeted, 1))

    def dec_copy(n, other):
        return pltpu.make_async_remote_copy(
            src_ref=dec.at[place], dst_ref=dec.at[place], send_sem=dec_s.at[n],
            recv_sem=dec_r.at[place], device_id={"seq": other, "head": hd}, device_id_type=MESH)

    def dec_arrival(other):
        slot = other % 4
        return pltpu.make_async_remote_copy(
            src_ref=dec.at[slot], dst_ref=dec.at[slot], send_sem=dec_s.at[0],
            recv_sem=dec_r.at[slot], device_id={"seq": other, "head": hd}, device_id_type=MESH)

    for n, other in enumerate((mate, across, diagonal)):
        dec_copy(n, other).start()

    def send(src, dst, ssem, rsem, s, h=None):
        return pltpu.make_async_remote_copy(
            src_ref=src, dst_ref=dst, send_sem=ssem, recv_sem=rsem,
            device_id={"seq": s, "head": hd if h is None else h}, device_id_type=MESH)

    def a_copy(i):
        return send(a_own.at[oth0 + i], a_oth.at[i], a_s.at[i], a_r.at[i], mate)

    def part(r):
        return pl.ds(r * (kd // 2), kd // 2)

    def x_copy(i, r):
        n = 2 * i + r
        return send(x_own.at[i, part(r)], x_nbr.at[i, part(r)], x_s.at[n], x_r.at[n], across)

    def z_copy(i, r):
        n = 2 * i + r
        return send(p_out.at[i, part(r)], p_in.at[i, part(r)], z_s.at[n], z_r.at[n],
                    jnp.minimum(seq + 4, n_seq - 4 + place))

    def i_copy(i):
        return send(i_oth.at[i], i_rcv.at[i], i_s.at[i], i_r.at[i], mate)

    def f_copy(i):
        oh, os_, slot = owner_of(i)
        return send(p_out.at[i], fin.at[slot], f_s.at[i], f_r.at[slot], os_, oh)

    def lanes(h):
        return pl.ds(pl.multiple_of(h * kd, kd), kd)

    def local_state(h):
        col = column(cum, h)
        scale = jnp.where(valid_col, jnp.exp(col[group - 1:group, :] - col), 0.0)
        wk = (k_vm[:, lanes(h)].astype(F32) * scale).astype(BF16)
        return lax.dot_general(
            wk, v_vm[:, lanes(h)], (((0,), (0,)), ((), ())), preferred_element_type=F32)

    def wait_loads(i, which):
        @pl.when(i % CHUNK == 0)
        def _():
            c = i // CHUNK * CHUNK
            for w in which:
                loads(oth0 + c, w).wait()
                loads(own0 + c, w).wait()

    def produce(i):
        wait_loads(i, (0, 1))
        one, two = local_state(oth0 + i), local_state(own0 + i)
        a_own[oth0 + i] = one
        a_copy(i).start()
        a_own[own0 + i] = two

    def combine(i):
        h = own0 + i
        a_copy(i).wait_recv()
        mine, theirs = a_own[h], a_oth[i]
        early = jnp.where(core == 0, mine, theirs)
        late = jnp.where(core == 0, theirs, mine)
        x_own[i] = early * dec[2 * xx + 1, pl.ds(h, 1), :] + late
        for r in range(2):
            x_copy(i, r).start()

    def chain(i, r):
        h = own0 + i
        x_copy(i, r).wait_recv()

        @pl.when(zz > 0)
        def _():
            z_copy(i, r).wait_recv()

        first = xx == 0
        at = part(r)
        mine, theirs = x_own[i, at], x_nbr[i, at]
        d0 = dec[0, pl.ds(h, 1), :] * dec[1, pl.ds(h, 1), :]
        d1 = dec[2, pl.ds(h, 1), :] * dec[3, pl.ds(h, 1), :]
        entering = p_in[i, at]
        middle = entering * d0 + jnp.where(first, mine, theirs)
        p_out[i, at] = middle * d1 + jnp.where(first, theirs, mine)

        @pl.when(zz < planes - 1)
        def _():
            z_copy(i, r).start()

        if r == 1:
            @pl.when(jnp.logical_and(zz == planes - 1, xx == i % 2))
            def _():
                oh, os_, slot = owner_of(i)
                away = jnp.logical_or(oh != hd, os_ != seq)

                @pl.when(away)
                def _():
                    f_copy(i).start()

                @pl.when(jnp.logical_not(away))
                def _():
                    fin[slot] = p_out[i]

        early = jnp.where(core == 0, a_own[h, at], a_oth[i, at])
        into0 = jnp.where(first, entering, middle)
        into1 = into0 * dec[2 * xx, pl.ds(h, 1), :] + early
        i_oth[i, at] = jnp.where(core == 0, into1, into0)
        if r == 1:
            i_copy(i).start()
        i_own[i, at] = jnp.where(core == 0, into0, into1)

    def inside(h):
        col = column(cum, h)
        row = cum_t[pl.ds(h, 1), :]
        blocks = []
        for lo in (0, group // 2):
            hi = lo + group // 2
            scores = lax.dot_general(
                q_vm[lo:hi, lanes(h)], k_vm[:hi, lanes(h)], (((1,), (1,)), ((), ())),
                preferred_element_type=F32)
            spread = col[lo:hi] - row[:, :hi]
            t_pos = lax.broadcasted_iota(jnp.int32, (hi - lo, hi), 0) + lo
            s_pos = lax.broadcasted_iota(jnp.int32, (hi - lo, hi), 1)
            keep = jnp.logical_and(t_pos >= s_pos, valid_row[:, :hi])
            weights = (scores * jnp.exp(jnp.where(keep, spread, -jnp.inf))).astype(BF16)
            blocks.append(jnp.dot(weights, v_vm[:hi, lanes(h)], preferred_element_type=F32))
        return jnp.concatenate(blocks, axis=0)

    def inside_pair(i):
        wait_loads(i, (2,))
        one, two = inside(own0 + i), inside(oth0 + i)
        intra[own0 + i] = one
        intra[oth0 + i] = two

    def finish(h, state):
        inter = jnp.exp(column(cum, h)) * jnp.dot(
            q_vm[:, lanes(h)], state.astype(BF16), preferred_element_type=F32)
        normed = head_norm(inter + intra[h], gain_ref[pl.ds(h, 1), :])
        return jnp.where(valid_col, normed, 0.0).astype(BF16)

    def put(h, block):
        o_vm[0, :, lanes(h)] = block

    lag = 4 + 2 * jnp.minimum(zz, 3)

    def round_of(n, c):
        i = n - lag
        running = jnp.logical_and(i >= 0, i < half)

        @pl.when(n < half)
        def _():
            produce(n)

        @pl.when(n == LAG - 1)
        def _():
            for other in (mate, across, diagonal):
                dec_arrival(other).wait_recv()

        @pl.when(jnp.logical_and(n >= LAG, n < half + LAG))
        def _():
            combine(n - LAG)

        @pl.when(running)
        def _():
            chain(i, 0)

        @pl.when(jnp.logical_and(n >= AHEAD, n < half + AHEAD))
        def _():
            inside_pair(n - AHEAD)

        @pl.when(running)
        def _():
            chain(i, 1)

        @pl.when(i == 0)
        def _():
            put(own0, finish(own0, i_own[0]))

        @pl.when(jnp.logical_and(i > 0, i < half))
        def _():
            i_copy(i - 1).wait_recv()
            one = finish(own0 + i, i_own[i])
            two = finish(oth0 + i - 1, i_rcv[i - 1])
            put(own0 + i, one)
            put(oth0 + i - 1, two)

        return c

    for copy in small[1:]:
        copy.wait()
    lax.fori_loop(0, half + lag, round_of, 0)
    i_copy(half - 1).wait_recv()
    put(oth0 + half - 1, finish(oth0 + half - 1, i_rcv[half - 1]))

    for p in range(rows):
        s, b, h = source_of(p)

        @pl.when(jnp.logical_or(s != seq, b != hd))
        def _():
            send(fin.at[p], fin.at[p], f_s.at[0], f_r.at[p], s, b).wait_recv()

        gain_row = gain_ref[pl.ds(h, 1), :]
        sk, sv, sq = sk_ref[p].astype(F32), sv_ref[p].astype(F32), sq_ref[p].astype(F32)
        now = fin[p]
        outs = []
        for j in range(sk.shape[0]):
            kcol = jnp.broadcast_to(sk[j:j + 1, :], (vd, kd)).T
            qcol = jnp.broadcast_to(sq[j:j + 1, :], (vd, kd)).T
            now = jnp.exp(jnp.broadcast_to(sgate_ref[p:p + 1, j:j + 1], (1, vd))) * now + kcol * sv[j:j + 1, :]
            outs.append(head_norm(jnp.sum(qcol * now, axis=0, keepdims=True), gain_row))
        step_ref[p] = jnp.concatenate(outs, axis=0).astype(BF16)
        cache_ref[p] = now

    for n, other in enumerate((mate, across, diagonal)):
        dec_copy(n, other).wait_send()

    def drain(i, c):
        a_copy(i).wait_send()
        i_copy(i).wait_send()
        for r in range(2):
            x_copy(i, r).wait_send()

        @pl.when(zz < planes - 1)
        def _():
            for r in range(2):
                z_copy(i, r).wait_send()

        @pl.when(jnp.logical_and(zz == planes - 1, xx == i % 2))
        def _():
            oh, os_, _slot = owner_of(i)

            @pl.when(jnp.logical_or(oh != hd, os_ != seq))
            def _():
                f_copy(i).wait_send()

        return c

    lax.fori_loop(0, half, drain, 0)


def store_kernel(*refs):
    n = len(refs) // 2
    copies = [pltpu.make_async_copy(refs[j], refs[n + j], refs[-1].at[j]) for j in range(n)]
    for copy in copies:
        copy.start()
    for copy in copies:
        copy.wait()


def per_device(n_seq, n_head, pq, pk, pv, lg, ln, gain, sq, sk, sv, sg):
    batch, group, width = pq.shape
    assert batch == 1 and n_seq % 4 == 0
    heads = lg.shape[2]
    half = heads // 2
    kd = width // heads
    vd = gain.shape[1]
    rows = sq.shape[0]
    vm = pl.BlockSpec(memory_space=pltpu.VMEM)
    sm = pl.BlockSpec(memory_space=pltpu.SMEM)
    far = pl.BlockSpec(memory_space=pltpu.HBM)
    state = lambda n: pltpu.VMEM((n, kd, vd), F32)
    dma = lambda *n: pltpu.SemaphoreType.DMA(n)
    results = pl.pallas_call(
        functools.partial(kernel, n_seq, n_head),
        out_shape=(
            pltpu.VMEM((batch, group, heads * vd), BF16),
            pltpu.VMEM(sv.shape, BF16),
            pltpu.VMEM((rows, kd, vd), F32),
        ),
        in_specs=[sm] + [far] * 9,
        out_specs=(vm, vm, vm),
        scratch_shapes=[
            pltpu.VMEM((group, width), BF16),
            pltpu.VMEM((group, width), BF16),
            pltpu.VMEM((group, heads * vd), BF16),
            pltpu.VMEM((batch, heads, group), F32),
            pltpu.VMEM(gain.shape, F32),
            pltpu.VMEM(sq.shape, BF16),
            pltpu.VMEM(sk.shape, BF16),
            pltpu.VMEM(sv.shape, BF16),
            pltpu.VMEM(sg.shape, F32),
            pltpu.VMEM((heads, group, vd), F32),
            pltpu.VMEM((group, heads), F32),
            pltpu.VMEM((heads, group), F32),
            pltpu.VMEM((4, heads, vd), F32),
            state(heads), state(half), state(half), state(half), state(half), state(half),
            state(half), state(half), state(half), state(rows),
            dma(3, heads // CHUNK), dma(6), dma(3), dma(4),
            dma(half), dma(half), dma(heads), dma(heads), dma(heads), dma(heads),
            dma(half), dma(half), dma(half), dma(rows),
        ],
        compiler_params=pltpu.CompilerParams(
            collective_id=0, has_side_effects=True, vmem_limit_bytes=60 * 1024 * 1024),
    )(ln, pq, pk, pv, jnp.transpose(lg, (0, 2, 1)), gain, sq, sk, sv, sg)
    return pl.pallas_call(
        store_kernel,
        out_shape=tuple(jax.ShapeDtypeStruct(r.shape, r.dtype) for r in results),
        in_specs=[vm] * 3,
        out_specs=(far,) * 3,
        scratch_shapes=[dma(3)],
        compiler_params=pltpu.CompilerParams(vmem_limit_bytes=8 * 1024 * 1024),
    )(*results)


def solution(mesh):
    return jax.shard_map(
        functools.partial(per_device, mesh.shape["seq"], mesh.shape["head"]),
        mesh=mesh,
        in_specs=(
            P("head", "seq", None),
            P("head", "seq", None),
            P("head", "seq", None),
            P("head", "seq", None),
            P("head"),
            P(),
            P(("head", "seq"), None, None),
            P(("head", "seq"), None, None),
            P(("head", "seq"), None, None),
            P(("head", "seq"), None),
        ),
        out_specs=(
            P("head", "seq", None),
            P(("head", "seq"), None, None),
            P(("head", "seq"), None, None),
        ),
        check_vma=False,
    )
```
